32 devices in a mesh: dp: 4 (over y, x), tensor: 8 (over z, core).
Axes of the slice: x: 2, y: 2, z: 4, core: 2. Of those that a mesh axis runs over, the one named last changes fastest.
Arguments:
- grad_out: bfloat16 [4096, 8192], P(('dp', 'tensor')), may hold values from -6 to 6
- out_weight: bfloat16 [8192, 4096], P('dp', 'tensor'), may hold values from -0.0625 to 0.0625
- query: bfloat16 [4096, 4096], P('dp', 'tensor'), may hold values from -6 to 6, as said below
- keys: bfloat16 [4096, 256], P('dp'), may hold values from -6 to 6
- values: bfloat16 [4096, 256], P('dp'), may hold values from -6 to 6
- attended: bfloat16 [4096, 4096], P('dp', 'tensor'), may hold values from -6 to 6, as said below
- stats: float32 [32, 4096], P('tensor', 'dp'), as said below
Outputs:
- query_grad: bfloat16 [4096, 4096], P('dp', 'tensor')
- key_grad: bfloat16 [4096, 256], P('dp', 'tensor')
- value_grad: bfloat16 [4096, 256], P('dp', 'tensor')
- weight_grad: bfloat16 [8192, 4096], P('dp', 'tensor')
The draws below stay inside these ranges and needn't reach their ends.
Inputs may be any that keep to these rules, and one draw needn't show every extreme that they name: query, keys and values are independent draws. attended is the causal attention output of the given query, keys and values within each sequence of 1024 rows: query head h uses key head h // 16, scores scaled by 128 ** -0.5, softmax over keys at or before the query. stats[h, t] is the logarithm of the sum of exp(score) over the keys that row t of head h attends to, for the same scores.
All inputs are finite; a program needn't handle non-finite values.
Results may differ from the reference program's by a relative error of at most 0.013.
Values may be sent and summed in bfloat16 or wider, within the bound.
A program may use at most 192 MiB of HBM per device.

```python
import jax
import jax.numpy as jnp
from jax import lax

D = 8192
HD = 128
GROUP = 16
LEN = 1024
HEADS = 32
KV_HEADS = 2
TOKENS = 4096


def draw_inputs(key):
    key_query = jax.random.fold_in(key, 101)
    key_keys = jax.random.fold_in(key, 202)
    key_values = jax.random.fold_in(key, 303)
    query = jnp.clip(jax.random.normal(key_query, (TOKENS, HEADS * HD), jnp.float32), -6.0, 6.0)
    keys = jnp.clip(jax.random.normal(key_keys, (TOKENS, KV_HEADS * HD), jnp.float32), -6.0, 6.0)
    values = jnp.clip(jax.random.normal(key_values, (TOKENS, KV_HEADS * HD), jnp.float32), -6.0, 6.0)
    return (query.astype(jnp.bfloat16), keys.astype(jnp.bfloat16), values.astype(jnp.bfloat16))


def forward_pass(key):
    query, keys, values = draw_inputs(key)
    seq_count = TOKENS // LEN
    query_split = query.astype(jnp.float32).reshape(seq_count, LEN, KV_HEADS, GROUP, HD)
    query_split = query_split.transpose(0, 2, 3, 1, 4).reshape(seq_count * KV_HEADS, GROUP, LEN, HD)
    keys_split = keys.astype(jnp.float32).reshape(seq_count, LEN, KV_HEADS, HD)
    keys_split = keys_split.transpose(0, 2, 1, 3).reshape(seq_count * KV_HEADS, LEN, HD)
    values_split = values.astype(jnp.float32).reshape(seq_count, LEN, KV_HEADS, HD)
    values_split = values_split.transpose(0, 2, 1, 3).reshape(seq_count * KV_HEADS, LEN, HD)
    positions = jnp.arange(LEN, dtype=jnp.int32)
    causal = positions[:, None] >= positions[None, :]

    def single(inputs):
        query_group, key_one, value_one = inputs
        scores = jnp.einsum('gqd,kd->gqk', query_group, key_one) * HD ** (-0.5)
        masked = jnp.where(causal[None], scores, -1e+30)
        highest = jnp.max(masked, axis=2, keepdims=True)
        log_total = highest[:, :, 0] + jnp.log(jnp.sum(jnp.exp(masked - highest), axis=2))
        weights_soft = jnp.exp(masked - log_total[:, :, None])
        output = jnp.einsum('gqk,kd->gqd', weights_soft, value_one)
        return (output, log_total)
    outputs, log_totals = lax.map(single, (query_split, keys_split, values_split))
    attended = outputs.reshape(seq_count, KV_HEADS, GROUP, LEN, HD).transpose(0, 3, 1, 2, 4)
    attended = attended.reshape(TOKENS, HEADS * HD)
    stats = log_totals.reshape(seq_count, KV_HEADS, GROUP, LEN).transpose(1, 2, 0, 3).reshape(HEADS, TOKENS)
    return (attended, stats)


def draw_query(key, part):
    return draw_inputs(key)[0]


def draw_keys(key, part):
    return draw_inputs(key)[1]


def draw_values(key, part):
    return draw_inputs(key)[2]


def draw_attended(key, part):
    return forward_pass(key)[0].astype(jnp.bfloat16)


def draw_stats(key, part):
    return forward_pass(key)[1].astype(jnp.float32)


def spiked(drawn, rng, source, target, shards_of, factor):
    owner, partner = [(jnp.arange(drawn.shape[dim]) // (drawn.shape[dim] // shards_of)).reshape([-1 if axis == dim else 1 for axis in range(drawn.ndim)]) for dim in (source, target)]
    chosen = jax.random.permutation(rng, shards_of)[partner]
    strong = (owner == chosen) | (owner == (partner + shards_of // 2) % shards_of)
    return jnp.where(strong, factor * drawn, drawn)


def block_levels(rng, dims, split, low, high):
    factor_of = 1.0
    for dim, blocks in split:
        heights = jax.random.uniform(jax.random.fold_in(jax.random.fold_in(rng, 6), dim), (blocks,), jnp.float32, low / len(split), high / len(split))
        factor_of = factor_of * jnp.repeat(jnp.exp(heights), dims[dim] // blocks).reshape((-1,) + (1,) * (len(dims) - 1 - dim))
    return factor_of


def noise(rng, dims, width, reach, cuts=(), kind=jnp.bfloat16):
    loudness = block_levels(rng, dims, cuts, -0.22, 0.18) if cuts else 1.0
    entries = jax.random.normal(rng, dims, jnp.float32) * width * loudness
    return jnp.minimum(jnp.maximum(entries, -reach), reach).astype(kind)


def gaussian_with(own_key, extent, deviation, reach, cuts, heavy, kind=jnp.bfloat16):
    entries = deviation * jax.random.normal(own_key, extent, jnp.float32)
    if cuts:
        entries = entries * block_levels(own_key, extent, cuts, -0.22, 0.18)
    return jnp.clip(spiked(entries, jax.random.fold_in(own_key, 3), *heavy), -reach, reach).astype(kind)


def setup_inputs(seed: int = 0) -> dict:
    key_of = jax.random.split(jax.random.key(seed), 8)
    return {
        "grad_out": gaussian_with(key_of[0], (TOKENS, D), 1.0, 6.0, ((0, 32),), (0, 1, 32, 2.75)),
        "out_weight": noise(key_of[1], (D, HEADS * HD), D ** -0.5, 0.0625, ((0, 4), (1, 8))),
        "query": draw_query(jax.random.fold_in(key_of[7], 71), 0),
        "keys": draw_keys(jax.random.fold_in(key_of[7], 71), 0),
        "values": draw_values(jax.random.fold_in(key_of[7], 71), 0),
        "attended": draw_attended(jax.random.fold_in(key_of[7], 71), 0),
        "stats": draw_stats(jax.random.fold_in(key_of[7], 71), 0),
    }


def split_heads(array, seq_count):
    shaped = array.reshape(seq_count, LEN, KV_HEADS, GROUP, HD).transpose(0, 2, 3, 1, 4)
    return shaped.reshape(seq_count * KV_HEADS, GROUP, LEN, HD)

def join_heads(array, seq_count):
    shaped = array.reshape(seq_count, KV_HEADS, GROUP, LEN, HD).transpose(0, 3, 1, 2, 4)
    return shaped.reshape(seq_count * LEN, KV_HEADS * GROUP * HD)

def split_keys(array, seq_count):
    shaped = array.reshape(seq_count, LEN, KV_HEADS, HD).transpose(0, 2, 1, 3)
    return shaped.reshape(seq_count * KV_HEADS, LEN, HD)

def join_keys(array, seq_count):
    shaped = array.reshape(seq_count, KV_HEADS, LEN, HD).transpose(0, 2, 1, 3)
    return shaped.reshape(seq_count * LEN, KV_HEADS * HD)

def head_grads(inputs):
    query_group, key_one, value_one, attended_group, grad_group, stats_group = inputs
    score_scale = HD ** (-0.5)
    query_wide = query_group.astype(jnp.float32)
    key_wide = key_one.astype(jnp.float32)
    grad_wide = grad_group.astype(jnp.float32)
    positions = jnp.arange(LEN, dtype=jnp.int32)
    causal = positions[:, None] >= positions[None, :]
    scores = jnp.einsum('gqd,kd->gqk', query_wide, key_wide) * score_scale
    attention = jnp.where(causal[None], jnp.exp(scores - stats_group[:, :, None]), 0.0)
    attention_low = lax.optimization_barrier(attention.astype(jnp.bfloat16)).astype(jnp.float32)
    grad_attention = jnp.einsum('gqd,kd->gqk', grad_wide, value_one.astype(jnp.float32))
    row_offset = lax.optimization_barrier(jnp.sum(grad_wide * attended_group.astype(jnp.float32), axis=2))
    grad_scores = attention * (grad_attention - row_offset[:, :, None])
    grad_scores = lax.optimization_barrier(grad_scores.astype(jnp.bfloat16)).astype(jnp.float32)
    query_grad = (jnp.einsum('gqk,kd->gqd', grad_scores, key_wide) * score_scale).astype(jnp.bfloat16)
    key_grad = (jnp.einsum('gqk,gqd->kd', grad_scores, query_wide) * score_scale).astype(jnp.bfloat16)
    value_grad = jnp.einsum('gqk,gqd->kd', attention_low, grad_wide).astype(jnp.bfloat16)
    return (query_grad, key_grad, value_grad)

def reference(grad_out, out_weight, query, keys, values, attended, stats):
    seq_count = TOKENS // LEN
    grad_att = jnp.dot(grad_out, out_weight, preferred_element_type=jnp.float32).astype(jnp.bfloat16)
    grad_seqs = grad_out.reshape(seq_count, LEN, D)
    attended_seqs = attended.reshape(seq_count, LEN, HEADS * HD)

    def add_grad(running, pair):
        grad_block, attended_block = pair
        grad_term = lax.dot_general(grad_block, attended_block, (((0,), (0,)), ((), ())), preferred_element_type=jnp.float32)
        rounded = lax.optimization_barrier(grad_term.astype(jnp.bfloat16))
        return (running + rounded.astype(jnp.float32), None)
    weight_sum, _ = lax.scan(add_grad, jnp.zeros((D, HEADS * HD), jnp.float32), (grad_seqs, attended_seqs))
    weight_grad = weight_sum.astype(jnp.bfloat16)
    stats_split = stats.reshape(KV_HEADS, GROUP, seq_count, LEN).transpose(2, 0, 1, 3)
    stats_split = stats_split.reshape(seq_count * KV_HEADS, GROUP, LEN)
    query_parts, key_parts, value_parts = lax.map(head_grads, (split_heads(query, seq_count), split_keys(keys, seq_count), split_keys(values, seq_count), split_heads(attended, seq_count), split_heads(grad_att, seq_count), stats_split))
    query_grad = join_heads(query_parts, seq_count)
    key_grad = join_keys(key_parts, seq_count)
    value_grad = join_keys(value_parts, seq_count)
    return (query_grad, key_grad, value_grad, weight_grad)
```

```python
import functools

import jax
import jax.numpy as jnp
from jax import lax
from jax.experimental import pallas as pl
from jax.experimental.pallas import tpu as pltpu
from jax.sharding import PartitionSpec as P

HD = 128
GROUP = 16
MESH = pl.DeviceIdType.MESH


def partner(value, axis, mask):
    pairs = [(source, source ^ mask) for source in range(lax.axis_size(axis))]
    return lax.ppermute(value, axis, pairs)


def nt_dot(a, b):
    return lax.dot_general(a, b, (((1,), (1,)), ((), ())), preferred_element_type=jnp.float32)


def attention_kernel(block, q_ref, k_ref, kt_ref, v_ref, o_ref, g_ref, s_ref, dq_ref, dkt_ref, dvt_ref, dk_ref, dv_ref):
    head = pl.program_id(0)
    length = q_ref.shape[0]
    scale = HD ** (-0.5)

    @pl.when(head == 0)
    def _():
        dk_ref[...] = jnp.zeros_like(dk_ref)
        dv_ref[...] = jnp.zeros_like(dv_ref)

    ones = jnp.ones((8, HD), jnp.float32)
    for j in range(length // block):
        rows = pl.ds(j * block, block)
        span = (j + 1) * block
        q = q_ref[rows, :]
        g = g_ref[rows, :]
        product = g.astype(jnp.float32) * o_ref[rows, :].astype(jnp.float32)
        offset = lax.dot_general(
            ones, product, (((1,), (1,)), ((), ())),
            preferred_element_type=jnp.float32, precision=lax.Precision.HIGHEST,
        )[:1, :]
        stat = s_ref[pl.ds(head, 1), rows]
        scores = nt_dot(k_ref[:span, :], q) * scale
        key_pos = lax.broadcasted_iota(jnp.int32, (span, block), 0)
        query_pos = lax.broadcasted_iota(jnp.int32, (span, block), 1) + j * block
        attention = jnp.where(key_pos <= query_pos, jnp.exp(scores - stat), 0.0)
        grad_attention = nt_dot(v_ref[:span, :], g)
        grad_scores = (attention * (grad_attention - offset)).astype(jnp.bfloat16)
        dv_ref[:span, :] += jnp.dot(
            attention.astype(jnp.bfloat16), g, preferred_element_type=jnp.float32
        )
        dk_ref[:span, :] += jnp.dot(grad_scores, q, preferred_element_type=jnp.float32)
        dq_t = jnp.dot(kt_ref[:, :span], grad_scores, preferred_element_type=jnp.float32)
        dq_ref[rows, :] = (dq_t * scale).T.astype(dq_ref.dtype)

    @pl.when(head == pl.num_programs(0) - 1)
    def _():
        dkt_ref[...] = (dk_ref[...] * scale).T
        dvt_ref[...] = dv_ref[...].T


def attention_grads(query, key_one, value_one, attended, grad_att, stats):
    length, width = query.shape
    heads = width // HD
    per_head = pl.BlockSpec((length, HD), lambda h: (0, h))
    shared = pl.BlockSpec((length, HD), lambda h: (0, 0))
    flat = pl.BlockSpec((HD, length), lambda h: (0, 0))
    return pl.pallas_call(
        functools.partial(attention_kernel, 256),
        grid=(heads,),
        in_specs=[
            per_head,
            shared,
            flat,
            shared,
            per_head,
            per_head,
            pl.BlockSpec((heads, length), lambda h: (0, 0)),
        ],
        out_specs=[per_head, flat, flat],
        scratch_shapes=[pltpu.VMEM((length, HD), jnp.float32)] * 2,
        out_shape=[
            jax.ShapeDtypeStruct((length, width), jnp.bfloat16),
            jax.ShapeDtypeStruct((HD, length), jnp.float32),
            jax.ShapeDtypeStruct((HD, length), jnp.float32),
        ],
        compiler_params=pltpu.CompilerParams(
            dimension_semantics=("arbitrary",), vmem_limit_bytes=40 * 2**20
        ),
        cost_estimate=pl.CostEstimate(
            flops=10 * heads * length * length * HD,
            bytes_accessed=10 * length * width,
            transcendentals=heads * length * length,
        ),
        name="attention_grads",
    )(query, key_one, key_one.T, value_one, attended, grad_att, stats)


def projection_plain(grad_out, out_weight, attended):
    grad_rows = lax.all_gather(grad_out, "tensor", axis=0, tiled=True)
    grad_att = jnp.dot(
        grad_rows,
        lax.all_gather(out_weight, "dp", axis=0, tiled=True),
        preferred_element_type=jnp.float32,
    ).astype(jnp.bfloat16)
    weight_grad = lax.psum_scatter(
        lax.dot_general(
            grad_rows, attended, (((0,), (0,)), ((), ())), preferred_element_type=jnp.float32
        ).astype(jnp.bfloat16),
        "dp",
        scatter_dimension=0,
        tiled=True,
    )
    return grad_att, weight_grad


def tn_dot(a, b):
    return lax.dot_general(a, b, (((0,), (0,)), ((), ())), preferred_element_type=jnp.float32)


def fused_kernel(
    chips, g_hbm, w_hbm, q_hbm, k_hbm, v_hbm, a_hbm, s_hbm,
    dq_hbm, dk_out, dv_out, wg_hbm,
    big, att_all, w, q, k, v, kt, stats, own, part_out, part_in, ga, acc, wg,
    dq_acc, dq, dk, dv, kv_t, kv_out, kv_in, half, half_out, half_in,
    load_sem, g_sem, p_sem, a_sem, ga_sem, kv_sem,
    pair_send, right_send, left_send, first_send, a_send, ga_send, kv_send, dq_send, wg_send,
):
    dp = big.shape[1]
    unit, depth = big.shape[2], big.shape[3]
    local = unit // 2
    cols = w.shape[1]
    heads = cols // HD
    scale = HD ** (-0.5)
    last = 4 * chips
    me = lax.axis_index("dp")
    place = lax.axis_index("tensor")
    z, core = lax.div(place, 2), lax.rem(place, 2)
    mate = place + 1 - 2 * core
    my_y, my_x = lax.div(me, 2), lax.rem(me, 2)

    def other(j):
        return lax.rem(my_y + j // 2, 2) * 2 + lax.rem(my_x + j % 2, 2)

    def band(index, size):
        return pl.ds(pl.multiple_of(index * size, size), size)

    mine = pl.ds(pl.multiple_of(core * local, local), local)
    theirs = pl.ds(pl.multiple_of((1 - core) * local, local), local)

    def remote(source, target, send, recv, row, column):
        return pltpu.make_async_remote_copy(
            src_ref=source, dst_ref=target, send_sem=send, recv_sem=recv,
            device_id=(row, column), device_id_type=MESH,
        )

    key_head = lax.div(place * heads, GROUP)
    loads = [
        (g_hbm.at[:, band(me, depth)], big.at[z, me, mine, :], g_sem.at[z * dp + me]),
        (w_hbm, w, load_sem.at[0]),
        (a_hbm, att_all.at[me], load_sem.at[1]),
        (k_hbm.at[:, band(key_head, HD)], k, load_sem.at[2]),
        (v_hbm.at[:, band(key_head, HD)], v, load_sem.at[3]),
        (q_hbm, q, load_sem.at[4]),
        (s_hbm, stats, load_sem.at[5]),
    ]
    loads = [pltpu.make_async_copy(*each) for each in loads]
    for each in loads:
        each.start()

    barrier = pltpu.get_barrier_semaphore()

    def greet(row, column):
        pl.semaphore_signal(barrier, inc=1, device_id=(row, column), device_id_type=MESH)

    for j in range(1, dp):
        greet(other(j), place)
    greet(me, mate)

    @pl.when(z > 0)
    def _():
        greet(me, place - 2)

    @pl.when(z < chips - 1)
    def _():
        greet(me, place + 2)

    edge = (z == 0).astype(jnp.int32) + (z == chips - 1).astype(jnp.int32)
    pl.semaphore_wait(barrier, dp + 2 - edge)

    def first_copy(j):
        return remote(
            g_hbm.at[:, band(other(j), depth)], big.at[z, me, mine, :],
            first_send.at[j - 1], g_sem.at[z * dp + me], other(j), place,
        )

    def attended_copy(j, block):
        return remote(
            a_hbm.at[band(block, unit), :], att_all.at[me, band(block, unit), :],
            a_send.at[(j - 1) * chips + block], a_sem.at[me * chips + block], other(j), place,
        )

    for j in range(1, dp):
        first_copy(j).start()
    for j in range(1, dp):
        attended_copy(j, z).start()

    def block_of(stage, side):
        block = z + (2 * side - 1) * stage
        inside = jnp.logical_and(block >= 0, block < chips)
        return block, jnp.logical_and(inside, jnp.logical_or(stage > 0, side == 0))

    def order_of(block, sub):
        ends = jnp.logical_or(block == 0, block == chips - 1).astype(jnp.int32)
        j = lax.rem(sub + ends, dp)
        return j, lax.rem(my_y + lax.div(j, 2), 2) * 2 + lax.rem(my_x + lax.rem(j, 2), 2)

    def pair_copy(block, row):
        slot = block * dp + row
        chunk = big.at[block, row, mine, :]
        return remote(chunk, chunk, pair_send.at[slot], p_sem.at[slot], me, mate)

    def right_copy(block, row):
        slot = block * dp + row
        chunk = big.at[block, row, mine, :]
        return remote(chunk, chunk, right_send.at[slot], g_sem.at[slot], me, place + 2)

    def left_copy(block, row):
        slot = block * dp + row
        chunk = big.at[block, row, mine, :]
        return remote(chunk, chunk, left_send.at[slot], g_sem.at[slot], me, place - 2)

    def part_copy(j, block, row):
        slot = (j - 1) * chips + block
        return remote(
            part_out.at[j - 1, band(block, unit), :], part_in.at[j - 1, band(block, unit), :],
            ga_send.at[slot], ga_sem.at[slot], row, place,
        )

    def sides(stage, sub, body):
        def step(side, carry):
            block, valid = block_of(stage, side)

            @pl.when(valid)
            def _():
                j, row = order_of(block, sub)
                body(side, block, j, row)

            return carry

        lax.fori_loop(0, 2, step, 0)

    def arrive(stage):
        def body(side, block, j, row):
            pair = pair_copy(block, row)
            slot = block * dp + row
            chunk = big.at[block, row, mine, :]
            remote(chunk, chunk, pair_send.at[slot], g_sem.at[slot], me, mate).wait_recv()

            @pl.when(jnp.logical_and(side == 0, z < chips - 1))
            def _():
                right_copy(block, row).start()

            @pl.when(jnp.logical_and(jnp.logical_or(side == 1, stage == 0), z > 0))
            def _():
                left_copy(block, row).start()

            pair.start()

        return body

    def project(side, block, j, row):
        slot = block * dp + row
        chunk = big.at[block, row, theirs, :]
        remote(chunk, chunk, pair_send.at[slot], p_sem.at[slot], me, mate).wait_recv()
        part = jnp.dot(big[block, row], w[...], preferred_element_type=jnp.float32)

        @pl.when(j == 0)
        def _():
            own[band(block, unit), :] = part

        @pl.when(j > 0)
        def _():
            part_out[j - 1, band(block, unit), :] = part.astype(jnp.bfloat16)

    def send_part(side, block, j, row):
        @pl.when(j > 0)
        def _():
            part_copy(j, block, row).start()

    def weight_term(side, block, j, row):
        @pl.when(j > 0)
        def _():
            rows = att_all.at[row, band(block, unit), :]
            slot = row * chips + block
            remote(rows, rows, a_send.at[0], a_sem.at[slot], me, mate).wait_recv()

        acc[...] += tn_dot(big[block, row], att_all[row, band(block, unit), :])

    ones = jnp.ones((8, HD), jnp.float32)

    def attend(side, block, _j, _row):
        rows = band(block, unit)
        total = own[rows, :]
        for j in range(1, dp):
            part_copy(j, block, me).wait_recv()
            total = total + part_in[j - 1, rows, :].astype(jnp.float32)
        ga[...] = total.astype(jnp.bfloat16)
        dq_acc[...] = jnp.zeros_like(dq_acc)
        offsets = []
        for h in range(heads):
            span = slice(h * HD, (h + 1) * HD)
            product = ga[:, span].astype(jnp.float32) * att_all[me, rows, span].astype(jnp.float32)
            offsets.append(
                lax.dot_general(
                    ones, product, (((1,), (1,)), ((), ())),
                    preferred_element_type=jnp.float32, precision=lax.Precision.HIGHEST,
                )[:1, :]
            )
        low = [stats[h : h + 1, rows] for h in range(heads)]

        def keys_step(tile, carry):
            keys = band(tile, unit)
            k_tile, v_tile, kt_tile = k[keys, :], v[keys, :], kt[:, keys]
            key_pos = lax.broadcasted_iota(jnp.int32, (unit, unit), 0) + tile * unit
            query_pos = lax.broadcasted_iota(jnp.int32, (unit, unit), 1) + block * unit
            allowed = key_pos <= query_pos
            dk_term, dv_term = dk[keys, :], dv[keys, :]
            for h in range(heads):
                span = slice(h * HD, (h + 1) * HD)
                q_tile, g_tile = q[rows, span], ga[:, span]
                scores = nt_dot(k_tile, q_tile) * scale
                attention = jnp.where(allowed, jnp.exp(scores - low[h]), 0.0)
                grad_attention = nt_dot(v_tile, g_tile)
                grad_scores = (attention * (grad_attention - offsets[h])).astype(jnp.bfloat16)
                dv_term += jnp.dot(
                    attention.astype(jnp.bfloat16), g_tile, preferred_element_type=jnp.float32
                )
                dk_term += jnp.dot(grad_scores, q_tile, preferred_element_type=jnp.float32)
                dq_acc[h] += jnp.dot(kt_tile, grad_scores, preferred_element_type=jnp.float32)
            dk[keys, :] = dk_term
            dv[keys, :] = dv_term
            return carry

        lax.fori_loop(0, block + 1, keys_step, 0)
        for h in range(heads):
            dq[rows, h * HD : (h + 1) * HD] = (dq_acc[h] * scale).T.astype(dq.dtype)
        pltpu.make_async_copy(dq.at[rows, :], dq_hbm.at[rows, :], dq_send.at[block]).start()

    for each in loads[1:]:
        each.wait()
    kt[...] = k[...].astype(jnp.float32).T.astype(jnp.bfloat16)
    acc[...] = jnp.zeros_like(acc)
    dk[...] = jnp.zeros_like(dk)
    dv[...] = jnp.zeros_like(dv)

    def round_of(index, carry):
        stage, sub = lax.div(index, dp), lax.rem(index, dp)

        @pl.when(index > 0)
        def _():
            sides(lax.div(index - 1, dp), lax.rem(index - 1, dp), send_part)

        @pl.when(index < last)
        def _():
            sides(stage, sub, arrive(stage))

        @pl.when(jnp.logical_and(sub > 0, stage < chips - 1))
        def _():
            for side in range(2):
                block, valid = block_of(stage + 1, side)
                for j in range(1, dp):

                    @pl.when(jnp.logical_and(valid, sub == j))
                    def _(j=j, block=block):
                        attended_copy(j, block).start()

        @pl.when(index < last)
        def _():
            sides(stage, sub, project)

        attend_stage = (
            (index == 3 * dp).astype(jnp.int32)
            + 2 * (index == 3 * dp + 2).astype(jnp.int32)
            + 3 * (index == last).astype(jnp.int32)
        )

        @pl.when(jnp.logical_or(index == 2 * dp, attend_stage > 0))
        def _():
            sides(attend_stage, 0, attend)

        @pl.when(jnp.logical_and(index > dp, index < last))
        def _():
            sides(lax.div(index - 1, dp), lax.rem(index - 1, dp), weight_term)

        @pl.when(jnp.logical_and(index >= dp, index < 2 * dp))
        def _():
            sides(0, sub, weight_term)

        return carry

    lax.fori_loop(0, last + 1, round_of, 0)

    width = HD // 4
    length = q.shape[0]
    odd = lax.rem(z, 2)
    kv_t[0] = (dk[...] * scale).T
    kv_t[1] = dv[...].T

    def strip(high, low_bit):
        return pl.ds(pl.multiple_of((high * 2 + low_bit) * width, width), width)

    for kind in range(2):
        for high in range(2):
            kv_out[kind, high] = kv_t[kind, strip(high, 1 - core), :].astype(jnp.bfloat16)
    sides(chips - 1, dp - 1, weight_term)
    kv_one = remote(kv_out, kv_in, kv_send.at[0], kv_sem.at[0], me, mate)
    kv_one.start()
    pieces = 4
    piece = depth // pieces
    copies = []
    for index in range(pieces):
        rows = slice(index * piece, (index + 1) * piece)
        wg[rows, :] = acc[rows, :].astype(jnp.bfloat16)
        copies.append(pltpu.make_async_copy(wg.at[rows, :], wg_hbm.at[rows, :], wg_send.at[index]))
        copies[-1].start()
    kv_one.wait_recv()
    for kind in range(2):
        for high in range(2):
            half[kind, high] = kv_t[kind, strip(high, core), :] + kv_in[kind, high].astype(jnp.float32)
        half_out[kind] = half[kind, 1 - odd].astype(jnp.bfloat16)
    kv_two = remote(half_out, half_in, kv_send.at[1], kv_sem.at[1], me, place + 2 - 4 * odd)
    kv_two.start()

    def settle(slot, carry):
        block, row = lax.div(slot, dp), lax.rem(slot, dp)
        pair_copy(block, row).wait_send()

        @pl.when(jnp.logical_and(block <= z, z < chips - 1))
        def _():
            right_copy(block, row).wait_send()

        @pl.when(jnp.logical_and(block >= z, z > 0))
        def _():
            left_copy(block, row).wait_send()

        return carry

    lax.fori_loop(0, chips * dp, settle, 0)
    for j in range(1, dp):
        first_copy(j).wait_send()
        for block in range(chips):
            attended_copy(j, block).wait_send()
            part_copy(j, block, me).wait_send()
    for block in range(chips):
        rows = pl.ds(block * unit, unit)
        pltpu.make_async_copy(dq.at[rows, :], dq_hbm.at[rows, :], dq_send.at[block]).wait()
    for each in copies:
        each.wait()
    kv_one.wait_send()
    kv_two.wait_recv()
    dk_out[...] = (half[0, odd] + half_in[0].astype(jnp.float32)).astype(jnp.bfloat16)
    dv_out[...] = (half[1, odd] + half_in[1].astype(jnp.float32)).astype(jnp.bfloat16)
    kv_two.wait_send()


def fused(grad_out, out_weight, query, keys, values, attended, stats):
    dp, tensor = lax.axis_size("dp"), lax.axis_size("tensor")
    chips = tensor // 2
    local = grad_out.shape[0]
    unit = 2 * local
    depth, cols = out_weight.shape
    length = query.shape[0]
    heads = cols // HD
    width = HD // 4
    low, wide = jnp.bfloat16, jnp.float32
    dma = pltpu.SemaphoreType.DMA
    anywhere = pl.BlockSpec(memory_space=pl.ANY)
    local_memory = pl.BlockSpec(memory_space=pltpu.VMEM)
    slots = chips * dp
    scratch = [
        pltpu.VMEM((chips, dp, unit, depth), low),
        pltpu.VMEM((dp, length, cols), low),
        pltpu.VMEM((depth, cols), low),
        pltpu.VMEM((length, cols), low),
        pltpu.VMEM((length, HD), low),
        pltpu.VMEM((length, HD), low),
        pltpu.VMEM((HD, length), low),
        pltpu.VMEM((heads, length), wide),
        pltpu.VMEM((length, cols), wide),
        pltpu.VMEM((dp - 1, length, cols), low),
        pltpu.VMEM((dp - 1, length, cols), low),
        pltpu.VMEM((unit, cols), low),
        pltpu.VMEM((depth, cols), wide),
        pltpu.VMEM((depth, cols), low),
        pltpu.VMEM((heads, HD, unit), wide),
        pltpu.VMEM((length, cols), low),
        pltpu.VMEM((length, HD), wide),
        pltpu.VMEM((length, HD), wide),
        pltpu.VMEM((2, HD, length), wide),
        pltpu.VMEM((2, 2, width, length), low),
        pltpu.VMEM((2, 2, width, length), low),
        pltpu.VMEM((2, 2, width, length), wide),
        pltpu.VMEM((2, width, length), low),
        pltpu.VMEM((2, width, length), low),
        dma((6,)),
        dma((slots,)),
        dma((slots,)),
        dma((slots,)),
        dma(((dp - 1) * chips,)),
        dma((2,)),
        dma((slots,)),
        dma((slots,)),
        dma((slots,)),
        dma((dp - 1,)),
        dma(((dp - 1) * chips,)),
        dma(((dp - 1) * chips,)),
        dma((2,)),
        dma((chips,)),
        dma((4,)),
    ]
    return pl.pallas_call(
        functools.partial(fused_kernel, chips),
        in_specs=[anywhere] * 7,
        out_specs=[anywhere, local_memory, local_memory, anywhere],
        out_shape=[
            jax.ShapeDtypeStruct((length, cols), low),
            jax.ShapeDtypeStruct((width, length), low),
            jax.ShapeDtypeStruct((width, length), low),
            jax.ShapeDtypeStruct((depth, cols), low),
        ],
        scratch_shapes=scratch,
        compiler_params=pltpu.CompilerParams(
            collective_id=0, has_side_effects=True, vmem_limit_bytes=60 * 2**20
        ),
        cost_estimate=pl.CostEstimate(
            flops=4 * dp * length * depth * cols + 10 * length * length * cols,
            bytes_accessed=2 * slots * local * depth,
            transcendentals=heads * length * length,
        ),
        name="fused_grads",
    )(grad_out, out_weight, query, keys, values, attended, stats)


def per_device(grad_out, out_weight, query, keys, values, attended, stats):
    heads = query.shape[1] // HD
    if lax.axis_size("dp") == 4 and lax.axis_size("tensor") == 8 and heads * 4 == GROUP:
        query_grad, key_t, value_t, weight_grad = fused(
            grad_out, out_weight, query, keys, values, attended, stats
        )
        return (query_grad, key_t.T, value_t.T, weight_grad)
    grad_att, weight_grad = projection_plain(grad_out, out_weight, attended)
    tensor_index = lax.axis_index("tensor")
    key_head = tensor_index * heads // GROUP
    key_one = lax.dynamic_slice_in_dim(keys, key_head * HD, HD, 1)
    value_one = lax.dynamic_slice_in_dim(values, key_head * HD, HD, 1)
    query_grad, key_part, value_part = attention_grads(
        query, key_one, value_one, attended, grad_att, stats
    )
    group_span = GROUP // heads
    group_place = tensor_index % group_span
    width, length = HD // group_span, query.shape[0]
    running_kv = jnp.stack([key_part, value_part]).reshape(2, group_span, width, length)
    for bit_number in range(group_span.bit_length() - 1):
        pairs = running_kv.reshape(2, -1, 2, width, length)
        odd = (group_place >> bit_number) % 2 == 1
        kept = jnp.where(odd, pairs[:, :, 1], pairs[:, :, 0])
        sent = jnp.where(odd, pairs[:, :, 0], pairs[:, :, 1])
        running_kv = kept + partner(
            sent.astype(jnp.bfloat16), "tensor", 1 << bit_number
        ).astype(sent.dtype)
    key_grad = running_kv[0, 0].T.astype(jnp.bfloat16)
    value_grad = running_kv[1, 0].T.astype(jnp.bfloat16)
    return (query_grad, key_grad, value_grad, weight_grad)


def solution(mesh):
    placed = (
        P(("dp", "tensor"), None),
        P("dp", "tensor"),
        P("dp", "tensor"),
        P("dp", None),
        P("dp", None),
        P("dp", "tensor"),
        P("tensor", "dp"),
    )
    return jax.shard_map(
        per_device,
        mesh=mesh,
        in_specs=placed,
        out_specs=(P("dp", "tensor"), P("dp", "tensor"), P("dp", "tensor"), P("dp", "tensor")),
        check_vma=False,
    )
```

```python
import functools

import jax
import jax.numpy as jnp
from jax import lax
from jax.experimental import pallas as pl
from jax.experimental.pallas import tpu as pltpu
from jax.sharding import PartitionSpec as P

HD = 128
GROUP = 16
MESH = pl.DeviceIdType.MESH


def partner(value, axis, mask):
    pairs = [(source, source ^ mask) for source in range(lax.axis_size(axis))]
    return lax.ppermute(value, axis, pairs)


def nt_dot(a, b):
    return lax.dot_general(a, b, (((1,), (1,)), ((), ())), preferred_element_type=jnp.float32)


def attention_kernel(block, q_ref, k_ref, kt_ref, v_ref, o_ref, g_ref, s_ref, dq_ref, dkt_ref, dvt_ref, dk_ref, dv_ref):
    head = pl.program_id(0)
    length = q_ref.shape[0]
    scale = HD ** (-0.5)

    @pl.when(head == 0)
    def _():
        dk_ref[...] = jnp.zeros_like(dk_ref)
        dv_ref[...] = jnp.zeros_like(dv_ref)

    ones = jnp.ones((8, HD), jnp.float32)
    for j in range(length // block):
        rows = pl.ds(j * block, block)
        span = (j + 1) * block
        q = q_ref[rows, :]
        g = g_ref[rows, :]
        product = g.astype(jnp.float32) * o_ref[rows, :].astype(jnp.float32)
        offset = lax.dot_general(
            ones, product, (((1,), (1,)), ((), ())),
            preferred_element_type=jnp.float32, precision=lax.Precision.HIGHEST,
        )[:1, :]
        stat = s_ref[pl.ds(head, 1), rows]
        scores = nt_dot(k_ref[:span, :], q) * scale
        key_pos = lax.broadcasted_iota(jnp.int32, (span, block), 0)
        query_pos = lax.broadcasted_iota(jnp.int32, (span, block), 1) + j * block
        attention = jnp.where(key_pos <= query_pos, jnp.exp(scores - stat), 0.0)
        grad_attention = nt_dot(v_ref[:span, :], g)
        grad_scores = (attention * (grad_attention - offset)).astype(jnp.bfloat16)
        dv_ref[:span, :] += jnp.dot(
            attention.astype(jnp.bfloat16), g, preferred_element_type=jnp.float32
        )
        dk_ref[:span, :] += jnp.dot(grad_scores, q, preferred_element_type=jnp.float32)
        dq_t = jnp.dot(kt_ref[:, :span], grad_scores, preferred_element_type=jnp.float32)
        dq_ref[rows, :] = (dq_t * scale).T.astype(dq_ref.dtype)

    @pl.when(head == pl.num_programs(0) - 1)
    def _():
        dkt_ref[...] = (dk_ref[...] * scale).T
        dvt_ref[...] = dv_ref[...].T


def attention_grads(query, key_one, value_one, attended, grad_att, stats):
    length, width = query.shape
    heads = width // HD
    per_head = pl.BlockSpec((length, HD), lambda h: (0, h))
    shared = pl.BlockSpec((length, HD), lambda h: (0, 0))
    flat = pl.BlockSpec((HD, length), lambda h: (0, 0))
    return pl.pallas_call(
        functools.partial(attention_kernel, 256),
        grid=(heads,),
        in_specs=[
            per_head,
            shared,
            flat,
            shared,
            per_head,
            per_head,
            pl.BlockSpec((heads, length), lambda h: (0, 0)),
        ],
        out_specs=[per_head, flat, flat],
        scratch_shapes=[pltpu.VMEM((length, HD), jnp.float32)] * 2,
        out_shape=[
            jax.ShapeDtypeStruct((length, width), jnp.bfloat16),
            jax.ShapeDtypeStruct((HD, length), jnp.float32),
            jax.ShapeDtypeStruct((HD, length), jnp.float32),
        ],
        compiler_params=pltpu.CompilerParams(
            dimension_semantics=("arbitrary",), vmem_limit_bytes=40 * 2**20
        ),
        cost_estimate=pl.CostEstimate(
            flops=10 * heads * length * length * HD,
            bytes_accessed=10 * length * width,
            transcendentals=heads * length * length,
        ),
        name="attention_grads",
    )(query, key_one, key_one.T, value_one, attended, grad_att, stats)


def projection_plain(grad_out, out_weight, attended):
    grad_rows = lax.all_gather(grad_out, "tensor", axis=0, tiled=True)
    grad_att = jnp.dot(
        grad_rows,
        lax.all_gather(out_weight, "dp", axis=0, tiled=True),
        preferred_element_type=jnp.float32,
    ).astype(jnp.bfloat16)
    weight_grad = lax.psum_scatter(
        lax.dot_general(
            grad_rows, attended, (((0,), (0,)), ((), ())), preferred_element_type=jnp.float32
        ).astype(jnp.bfloat16),
        "dp",
        scatter_dimension=0,
        tiled=True,
    )
    return grad_att, weight_grad


def tn_dot(a, b):
    return lax.dot_general(a, b, (((0,), (0,)), ((), ())), preferred_element_type=jnp.float32)


def fused_kernel(
    chips, g_hbm, w_hbm, q_hbm, k_hbm, v_hbm, a_hbm, s_hbm,
    dq_hbm, dk_out, dv_out, wg_hbm,
    big, att_all, w, q, k, v, kt, stats, own, part_out, part_in, ga, acc, wg,
    dq_acc, dq, dk, dv, kv_t, kv_out, kv_in, kv_done,
    load_sem, half_sem, g_sem, p_sem, a_sem, ga_sem, kv_sem,
    pair_send, right_send, left_send, first_send, a_send, ga_send, kv_send, dq_send, wg_send,
):
    dp = big.shape[1]
    unit, depth = big.shape[2], big.shape[3]
    local = unit // 2
    cols = w.shape[1]
    heads = cols // HD
    scale = HD ** (-0.5)
    last = 4 * chips
    me = lax.axis_index("dp")
    place = lax.axis_index("tensor")
    z, core = lax.div(place, 2), lax.rem(place, 2)
    mate = place + 1 - 2 * core
    my_y, my_x = lax.div(me, 2), lax.rem(me, 2)

    def other(j):
        return lax.rem(my_y + j // 2, 2) * 2 + lax.rem(my_x + j % 2, 2)

    def band(index, size):
        return pl.ds(pl.multiple_of(index * size, size), size)

    mine = pl.ds(pl.multiple_of(core * local, local), local)
    theirs = pl.ds(pl.multiple_of((1 - core) * local, local), local)

    def remote(source, target, send, recv, row, column):
        return pltpu.make_async_remote_copy(
            src_ref=source, dst_ref=target, send_sem=send, recv_sem=recv,
            device_id=(row, column), device_id_type=MESH,
        )

    key_head = lax.div(place * heads, GROUP)
    loads = [
        (g_hbm.at[:, band(me, depth)], big.at[z, me, mine, :], g_sem.at[z * dp + me]),
        (w_hbm, w, load_sem.at[0]),
        (a_hbm, att_all.at[me], load_sem.at[1]),
        (k_hbm.at[:, band(key_head, HD)], k, load_sem.at[2]),
        (v_hbm.at[:, band(key_head, HD)], v, load_sem.at[3]),
        (q_hbm, q, load_sem.at[4]),
        (s_hbm, stats, load_sem.at[5]),
    ]
    loads = [pltpu.make_async_copy(*each) for each in loads]
    for each in loads:
        each.start()

    barrier = pltpu.get_barrier_semaphore()

    def greet(row, column):
        pl.semaphore_signal(barrier, inc=1, device_id=(row, column), device_id_type=MESH)

    for j in range(1, dp):
        greet(other(j), place)
    greet(me, mate)
    greet(me, place + 2 - 4 * lax.rem(z, 2) + 1 - 2 * core)

    @pl.when(z > 0)
    def _():
        greet(me, place - 2)

    @pl.when(z < chips - 1)
    def _():
        greet(me, place + 2)

    acc[...] = jnp.zeros_like(acc)
    dk[...] = jnp.zeros_like(dk)
    dv[...] = jnp.zeros_like(dv)
    with jax.named_scope("loads"):
        for each in loads[1:]:
            each.wait()
    kt[...] = k[...].astype(jnp.float32).T.astype(jnp.bfloat16)

    edge = (z == 0).astype(jnp.int32) + (z == chips - 1).astype(jnp.int32)
    with jax.named_scope("barrier"):
        pl.semaphore_wait(barrier, dp + 3 - edge)

    def first_copy(j):
        return remote(
            g_hbm.at[:, band(other(j), depth)], big.at[z, me, mine, :],
            first_send.at[j - 1], g_sem.at[z * dp + me], other(j), place,
        )

    def attended_copy(j, block):
        return remote(
            a_hbm.at[band(block, unit), :], att_all.at[me, band(block, unit), :],
            a_send.at[(j - 1) * chips + block], a_sem.at[me * chips + block], other(j), place,
        )

    def halves(part):
        return pl.ds(pl.multiple_of(core * local + part * (local // 2), local // 2), local // 2)

    def early_copy(part):
        return remote(
            g_hbm.at[pl.ds(part * (local // 2), local // 2), band(other(1), depth)],
            big.at[z, me, halves(part), :],
            first_send.at[(dp - 1) * part], half_sem if part else g_sem.at[z * dp + me],
            other(1), place,
        )

    early_copy(0).start()
    first_copy(2).start()
    early_copy(1).start()
    first_copy(3).start()
    for j in range(1, dp):
        attended_copy(j, z).start()

    def block_of(stage, side):
        block = z + (2 * side - 1) * stage
        inside = jnp.logical_and(block >= 0, block < chips)
        return block, jnp.logical_and(inside, jnp.logical_or(stage > 0, side == 0))

    def pair_copy(block, row):
        slot = block * dp + row
        chunk = big.at[block, row, mine, :]
        return remote(chunk, chunk, pair_send.at[slot], p_sem.at[slot], me, mate)

    def right_copy(block, row):
        slot = block * dp + row
        chunk = big.at[block, row, mine, :]
        return remote(chunk, chunk, right_send.at[slot], g_sem.at[slot], me, place + 2)

    def left_copy(block, row):
        slot = block * dp + row
        chunk = big.at[block, row, mine, :]
        return remote(chunk, chunk, left_send.at[slot], g_sem.at[slot], me, place - 2)

    def part_copy(j, block, row):
        slot = (j - 1) * chips + block
        return remote(
            part_out.at[j - 1, band(block, unit), :], part_in.at[j - 1, band(block, unit), :],
            ga_send.at[slot], ga_sem.at[slot], row, place,
        )

    def sides(stage, sub, body):
        def step(turn, carry):
            side = lax.select(jnp.logical_and(z == 1, stage > 0), 1 - turn, turn)
            block, valid = block_of(stage, side)

            @pl.when(valid)
            def _():
                swapped = jnp.logical_and(z == 0, stage > 1)
                place_of = (stage - 2) * dp + sub
                end = place_of == 2 * dp - 1
                early = jnp.logical_or(place_of < dp - 1, end)
                at = lax.select(swapped, lax.select(early, 2, 3), block)
                plain = lax.select(jnp.logical_or(at == 0, at == chips - 1), lax.rem(sub + 1, dp), sub)
                j = lax.select(
                    swapped,
                    lax.select(
                        end, 0,
                        lax.select(early, sub + 1, lax.rem(place_of - (dp - 1) + 1, dp)),
                    ),
                    plain,
                )
                row = lax.rem(my_y + lax.div(j, 2), 2) * 2 + lax.rem(my_x + lax.rem(j, 2), 2)
                body(side, at, j, row)

            return carry

        lax.fori_loop(0, 2, step, 0)

    def arrive(stage):
        def body(side, block, j, row):
            slot = block * dp + row
            held = jnp.logical_and(jnp.logical_and(z == 1, block == 2), j == 0)
            rightward = jnp.logical_and(side == 0, z < chips - 1)
            leftward = jnp.logical_and(jnp.logical_or(side == 1, stage == 0), z > 0)
            leftward = jnp.logical_and(leftward, jnp.logical_not(held))

            def pass_on(rows, sem):
                chunk = big.at[block, row, rows, :]
                with jax.named_scope("wait_chunk"):
                    remote(chunk, chunk, pair_send.at[slot], sem, me, mate).wait_recv()

                @pl.when(rightward)
                def _():
                    remote(chunk, chunk, right_send.at[slot], g_sem.at[slot], me, place + 2).start()

                @pl.when(leftward)
                def _():
                    remote(chunk, chunk, left_send.at[slot], g_sem.at[slot], me, place - 2).start()

            early = jnp.logical_and(stage == 0, j == 1)

            @pl.when(early)
            def _():
                pass_on(halves(0), g_sem.at[slot])
                pass_on(halves(1), half_sem)

            @pl.when(jnp.logical_not(early))
            def _():
                pass_on(mine, g_sem.at[slot])

            pair_copy(block, row).start()

        return body

    def project(side, block, j, row):
        slot = block * dp + row
        chunk = big.at[block, row, theirs, :]
        with jax.named_scope("wait_mate"):
            remote(chunk, chunk, pair_send.at[slot], p_sem.at[slot], me, mate).wait_recv()
        part = jnp.dot(big[block, row], w[...], preferred_element_type=jnp.float32)

        @pl.when(j == 0)
        def _():
            own[band(block, unit), :] = part

        @pl.when(j > 0)
        def _():
            part_out[j - 1, band(block, unit), :] = part.astype(jnp.bfloat16)

    def send_part(side, block, j, row):
        @pl.when(j > 0)
        def _():
            part_copy(j, block, row).start()

    def weight_term(side, block, j, row):
        @pl.when(j > 0)
        def _():
            rows = att_all.at[row, band(block, unit), :]
            slot = row * chips + block
            with jax.named_scope("wait_attended"):
                remote(rows, rows, a_send.at[0], a_sem.at[slot], me, mate).wait_recv()

        acc[...] += tn_dot(big[block, row], att_all[row, band(block, unit), :])

    ones = jnp.ones((8, HD), jnp.float32)

    width = HD // 4
    odd = lax.rem(z, 2)

    def strip(high, low_bit):
        return pl.ds(pl.multiple_of((high * 2 + low_bit) * width, width), width)

    beside = place + 2 - 4 * odd
    across = beside + 1 - 2 * core
    group = ((mate, odd, 1 - core), (beside, 1 - odd, core), (across, 1 - odd, 1 - core))

    def kv_store(tile):
        keys = band(tile, unit)
        kv_t[tile, 0] = (dk[keys, :] * scale).T
        kv_t[tile, 1] = dv[keys, :].T
        for number, (_, high, low_bit) in enumerate(group):
            for kind in range(2):
                kv_out[tile, number, kind] = kv_t[tile, kind, strip(high, low_bit), :].astype(jnp.bfloat16)

    def kv_copies(tile):
        return [
            remote(
                kv_out.at[tile, number], kv_in.at[tile, number],
                kv_send.at[tile * 3 + number], kv_sem.at[tile * 3 + number], me, peer,
            )
            for number, (peer, _, _) in enumerate(group)
        ]

    def kv_start(tile):
        for each in kv_copies(tile):
            each.start()

    final_block = lax.select(z == 0, 2, lax.select(z == 1, chips - 1, 0))

    def attend(block):
        rows = band(block, unit)
        total = own[rows, :]
        for j in range(1, dp):
            with jax.named_scope("wait_part"):
                part_copy(j, block, me).wait_recv()
            total = total + part_in[j - 1, rows, :].astype(jnp.float32)
        ga[...] = total.astype(jnp.bfloat16)
        dq_acc[...] = jnp.zeros_like(dq_acc)
        offsets = []
        for h in range(heads):
            span = slice(h * HD, (h + 1) * HD)
            product = ga[:, span].astype(jnp.float32) * att_all[me, rows, span].astype(jnp.float32)
            offsets.append(
                lax.dot_general(
                    ones, product, (((1,), (1,)), ((), ())),
                    preferred_element_type=jnp.float32, precision=lax.Precision.HIGHEST,
                )[:1, :]
            )
        low = [stats[h : h + 1, rows] for h in range(heads)]

        def keys_tile(tile):
            keys = band(tile, unit)
            k_tile, v_tile, kt_tile = k[keys, :], v[keys, :], kt[:, keys]
            key_pos = lax.broadcasted_iota(jnp.int32, (unit, unit), 0) + tile * unit
            query_pos = lax.broadcasted_iota(jnp.int32, (unit, unit), 1) + block * unit
            allowed = key_pos <= query_pos
            dk_term, dv_term = dk[keys, :], dv[keys, :]
            for h in range(heads):
                span = slice(h * HD, (h + 1) * HD)
                q_tile, g_tile = q[rows, span], ga[:, span]
                scores = nt_dot(k_tile, q_tile) * scale
                attention = jnp.where(allowed, jnp.exp(scores - low[h]), 0.0)
                grad_attention = nt_dot(v_tile, g_tile)
                grad_scores = (attention * (grad_attention - offsets[h])).astype(jnp.bfloat16)
                dv_term += jnp.dot(
                    attention.astype(jnp.bfloat16), g_tile, preferred_element_type=jnp.float32
                )
                dk_term += jnp.dot(grad_scores, q_tile, preferred_element_type=jnp.float32)
                dq_acc[h] += jnp.dot(kt_tile, grad_scores, preferred_element_type=jnp.float32)
            dk[keys, :] = dk_term
            dv[keys, :] = dv_term

        final = block == final_block
        def keys_step(tile, carry):
            keys_tile(tile)

            @pl.when(final)
            def _():
                kv_store(tile)

                @pl.when(tile >= 1)
                def _():
                    kv_start(tile - 1)

            return carry

        lax.fori_loop(0, block + 1, keys_step, 0)
        for h in range(heads):
            dq[rows, h * HD : (h + 1) * HD] = (dq_acc[h] * scale).T.astype(dq.dtype)
        pltpu.make_async_copy(dq.at[rows, :], dq_hbm.at[rows, :], dq_send.at[block]).start()

        @pl.when(final)
        def _():
            kv_start(block)

    def store_tile(tile, carry):
        kv_store(tile)
        return carry

    def start_tile(tile, carry):
        kv_start(tile)
        return carry

    def round_of(index, carry):
        @pl.when(index == last - 1)
        def _():
            lax.fori_loop(final_block + 1, chips, store_tile, 0)
            sides(chips - 1, dp - 2, weight_term)
            lax.fori_loop(final_block + 1, chips, start_tile, 0)

        stage, sub = lax.div(index, dp), lax.rem(index, dp)

        @pl.when(index < last)
        def _():
            sides(stage, sub, arrive(stage))

        @pl.when(jnp.logical_and(z == 1, index == 3 * dp - 1))
        def _():
            left_copy(2, me).start()

        @pl.when(jnp.logical_and(sub > 0, stage < chips - 1))
        def _():
            for side in range(2):
                block, valid = block_of(stage + 1, side)
                for j in range(1, dp):

                    @pl.when(jnp.logical_and(valid, sub == j))
                    def _(j=j, block=block):
                        attended_copy(j, block).start()

        @pl.when(index < last)
        def _():
            with jax.named_scope("project"):
                sides(stage, sub, project)

        @pl.when(jnp.logical_and(index > dp, index < last - 1))
        def _():
            with jax.named_scope("weight"):
                sides(lax.div(index - 1, dp), lax.rem(index - 1, dp), weight_term)

        @pl.when(jnp.logical_and(index >= dp, index < 2 * dp))
        def _():
            sides(0, sub, weight_term)

        @pl.when(index < last)
        def _():
            sides(stage, sub, send_part)

        attend_stage = (
            (index == 3 * dp).astype(jnp.int32)
            + 2 * (index == 3 * dp + 2).astype(jnp.int32)
            + 3 * (index == last).astype(jnp.int32)
        )

        @pl.when(jnp.logical_or(index == 2 * dp, attend_stage > 0))
        def _():
            with jax.named_scope("attend"):

                def step(side, carry):
                    block, valid = block_of(attend_stage, side)
                    swapped = lax.select(attend_stage == 2, 3, lax.select(attend_stage == 3, 2, attend_stage))

                    @pl.when(valid)
                    def _():
                        attend(lax.select(z == 0, swapped, block))

                    return carry

                lax.fori_loop(0, 2, step, 0)

        return carry

    lax.fori_loop(0, last + 1, round_of, 0)

    with jax.named_scope("weight_last"):
        sides(chips - 1, dp - 1, weight_term)
    pieces = 4
    piece = depth // pieces
    copies = []
    for index in range(pieces):
        rows = slice(index * piece, (index + 1) * piece)
        wg[rows, :] = acc[rows, :].astype(jnp.bfloat16)
        copies.append(pltpu.make_async_copy(wg.at[rows, :], wg_hbm.at[rows, :], wg_send.at[index]))
        copies[-1].start()

    def settle(slot, carry):
        block, row = lax.div(slot, dp), lax.rem(slot, dp)
        pair_copy(block, row).wait_send()

        @pl.when(jnp.logical_and(block <= z, z < chips - 1))
        def _():
            right_copy(block, row).wait_send()

        @pl.when(jnp.logical_and(block >= z, z > 0))
        def _():
            left_copy(block, row).wait_send()

        return carry

    with jax.named_scope("settle"):
        lax.fori_loop(0, chips * dp, settle, 0)
    for part in range(2):
        early_copy(part).wait_send()
    for j in range(1, dp):
        if j > 1:
            first_copy(j).wait_send()
        for block in range(chips):
            attended_copy(j, block).wait_send()
            part_copy(j, block, me).wait_send()
    for block in range(chips):
        rows = pl.ds(block * unit, unit)
        pltpu.make_async_copy(dq.at[rows, :], dq_hbm.at[rows, :], dq_send.at[block]).wait()
    for each in copies:
        each.wait()
    for tile in range(chips):
        for each in kv_copies(tile):
            with jax.named_scope("wait_kv"):
                each.wait_recv()
    with jax.named_scope("kv_sum"):
        for tile in range(chips):
            keys = slice(tile * unit, (tile + 1) * unit)
            for kind in range(2):
                total = kv_t[tile, kind, strip(odd, core), :]
                for number in range(3):
                    total = total + kv_in[tile, number, kind].astype(jnp.float32)
                kv_done[kind, :, keys] = total.astype(jnp.bfloat16)
    copies = [
        pltpu.make_async_copy(kv_done.at[kind], out, load_sem.at[kind])
        for kind, out in enumerate((dk_out, dv_out))
    ]
    for each in copies:
        each.start()
    for tile in range(chips):
        for each in kv_copies(tile):
            each.wait_send()
    for each in copies:
        each.wait()


def finish_kernel(*refs):
    sources, targets, buffers, sems = refs[:4], refs[4:8], refs[8:12], refs[12:]
    pieces = ((0, 4), (1, 1), (2, 1), (3, 8))
    moves = []
    for index, count in pieces:
        size = sources[index].shape[0] // count
        for part in range(count):
            rows = pl.ds(part * size, size)
            slot = len(moves)
            moves.append(
                (
                    pltpu.make_async_copy(
                        sources[index].at[rows, :], buffers[index].at[rows, :], sems[0].at[slot]
                    ),
                    pltpu.make_async_copy(
                        buffers[index].at[rows, :], targets[index].at[rows, :], sems[1].at[slot]
                    ),
                )
            )
    for into, _ in moves:
        into.start()
    for into, out in moves:
        into.wait()
        out.start()
    for _, out in moves:
        out.wait()


def finish(*arrays):
    anywhere = pl.BlockSpec(memory_space=pl.ANY)
    shapes = [jax.ShapeDtypeStruct(each.shape, each.dtype) for each in arrays]
    return pl.pallas_call(
        finish_kernel,
        in_specs=[anywhere] * 4,
        out_specs=[anywhere] * 4,
        out_shape=shapes,
        scratch_shapes=[pltpu.VMEM(each.shape, each.dtype) for each in arrays]
        + [pltpu.SemaphoreType.DMA((14,)), pltpu.SemaphoreType.DMA((14,))],
        name="finish",
    )(*arrays)


def fused(grad_out, out_weight, query, keys, values, attended, stats):
    dp, tensor = lax.axis_size("dp"), lax.axis_size("tensor")
    chips = tensor // 2
    local = grad_out.shape[0]
    unit = 2 * local
    depth, cols = out_weight.shape
    length = query.shape[0]
    heads = cols // HD
    width = HD // 4
    low, wide = jnp.bfloat16, jnp.float32
    dma = pltpu.SemaphoreType.DMA
    anywhere = pl.BlockSpec(memory_space=pl.ANY)
    slots = chips * dp
    scratch = [
        pltpu.VMEM((chips, dp, unit, depth), low),
        pltpu.VMEM((dp, length, cols), low),
        pltpu.VMEM((depth, cols), low),
        pltpu.VMEM((length, cols), low),
        pltpu.VMEM((length, HD), low),
        pltpu.VMEM((length, HD), low),
        pltpu.VMEM((HD, length), low),
        pltpu.VMEM((heads, length), wide),
        pltpu.VMEM((length, cols), wide),
        pltpu.VMEM((dp - 1, length, cols), low),
        pltpu.VMEM((dp - 1, length, cols), low),
        pltpu.VMEM((unit, cols), low),
        pltpu.VMEM((depth, cols), wide),
        pltpu.VMEM((depth, cols), low),
        pltpu.VMEM((heads, HD, unit), wide),
        pltpu.VMEM((length, cols), low),
        pltpu.VMEM((length, HD), wide),
        pltpu.VMEM((length, HD), wide),
        pltpu.VMEM((chips, 2, HD, unit), wide),
        pltpu.VMEM((chips, 3, 2, width, unit), low),
        pltpu.VMEM((chips, 3, 2, width, unit), low),
        pltpu.VMEM((2, width, length), low),
        dma((6,)),
        dma,
        dma((slots,)),
        dma((slots,)),
        dma((slots,)),
        dma(((dp - 1) * chips,)),
        dma((3 * chips,)),
        dma((slots,)),
        dma((slots,)),
        dma((slots,)),
        dma((dp,)),
        dma(((dp - 1) * chips,)),
        dma(((dp - 1) * chips,)),
        dma((3 * chips,)),
        dma((chips,)),
        dma((4,)),
    ]
    return pl.pallas_call(
        functools.partial(fused_kernel, chips),
        in_specs=[anywhere] * 7,
        out_specs=[anywhere] * 4,
        out_shape=[
            jax.ShapeDtypeStruct((length, cols), low),
            jax.ShapeDtypeStruct((width, length), low),
            jax.ShapeDtypeStruct((width, length), low),
            jax.ShapeDtypeStruct((depth, cols), low),
        ],
        scratch_shapes=scratch,
        compiler_params=pltpu.CompilerParams(
            collective_id=0, has_side_effects=True, vmem_limit_bytes=60 * 2**20
        ),
        cost_estimate=pl.CostEstimate(
            flops=4 * dp * length * depth * cols + 10 * length * length * cols,
            bytes_accessed=2 * slots * local * depth,
            transcendentals=heads * length * length,
        ),
        name="fused_grads",
    )(grad_out, out_weight, query, keys, values, attended, stats)


def per_device(grad_out, out_weight, query, keys, values, attended, stats):
    heads = query.shape[1] // HD
    if lax.axis_size("dp") == 4 and lax.axis_size("tensor") == 8 and heads * 4 == GROUP:
        query_grad, key_t, value_t, weight_grad = finish(
            *fused(grad_out, out_weight, query, keys, values, attended, stats)
        )
        return (query_grad, key_t.T, value_t.T, weight_grad)
    grad_att, weight_grad = projection_plain(grad_out, out_weight, attended)
    tensor_index = lax.axis_index("tensor")
    key_head = tensor_index * heads // GROUP
    key_one = lax.dynamic_slice_in_dim(keys, key_head * HD, HD, 1)
    value_one = lax.dynamic_slice_in_dim(values, key_head * HD, HD, 1)
    query_grad, key_part, value_part = attention_grads(
        query, key_one, value_one, attended, grad_att, stats
    )
    group_span = GROUP // heads
    group_place = tensor_index % group_span
    width, length = HD // group_span, query.shape[0]
    running_kv = jnp.stack([key_part, value_part]).reshape(2, group_span, width, length)
    for bit_number in range(group_span.bit_length() - 1):
        pairs = running_kv.reshape(2, -1, 2, width, length)
        odd = (group_place >> bit_number) % 2 == 1
        kept = jnp.where(odd, pairs[:, :, 1], pairs[:, :, 0])
        sent = jnp.where(odd, pairs[:, :, 0], pairs[:, :, 1])
        running_kv = kept + partner(
            sent.astype(jnp.bfloat16), "tensor", 1 << bit_number
        ).astype(sent.dtype)
    key_grad = running_kv[0, 0].T.astype(jnp.bfloat16)
    value_grad = running_kv[1, 0].T.astype(jnp.bfloat16)
    return (query_grad, key_grad, value_grad, weight_grad)


def solution(mesh):
    placed = (
        P(("dp", "tensor"), None),
        P("dp", "tensor"),
        P("dp", "tensor"),
        P("dp", None),
        P("dp", None),
        P("dp", "tensor"),
        P("tensor", "dp"),
    )
    return jax.shard_map(
        per_device,
        mesh=mesh,
        in_specs=placed,
        out_specs=(P("dp", "tensor"), P("dp", "tensor"), P("dp", "tensor"), P("dp", "tensor")),
        check_vma=False,
    )
```

```python
import functools

import jax
import jax.numpy as jnp
from jax import lax
from jax.experimental import pallas as pl
from jax.experimental.pallas import tpu as pltpu
from jax.sharding import PartitionSpec as P

HD = 128
GROUP = 16
MESH = pl.DeviceIdType.MESH


def partner(value, axis, mask):
    pairs = [(source, source ^ mask) for source in range(lax.axis_size(axis))]
    return lax.ppermute(value, axis, pairs)


def nt_dot(a, b):
    return lax.dot_general(a, b, (((1,), (1,)), ((), ())), preferred_element_type=jnp.float32)


def attention_kernel(block, q_ref, k_ref, kt_ref, v_ref, o_ref, g_ref, s_ref, dq_ref, dkt_ref, dvt_ref, dk_ref, dv_ref):
    head = pl.program_id(0)
    length = q_ref.shape[0]
    scale = HD ** (-0.5)

    @pl.when(head == 0)
    def _():
        dk_ref[...] = jnp.zeros_like(dk_ref)
        dv_ref[...] = jnp.zeros_like(dv_ref)

    ones = jnp.ones((8, HD), jnp.float32)
    for j in range(length // block):
        rows = pl.ds(j * block, block)
        span = (j + 1) * block
        q = q_ref[rows, :]
        g = g_ref[rows, :]
        product = g.astype(jnp.float32) * o_ref[rows, :].astype(jnp.float32)
        offset = lax.dot_general(
            ones, product, (((1,), (1,)), ((), ())),
            preferred_element_type=jnp.float32, precision=lax.Precision.HIGHEST,
        )[:1, :]
        stat = s_ref[pl.ds(head, 1), rows]
        scores = nt_dot(k_ref[:span, :], q) * scale
        key_pos = lax.broadcasted_iota(jnp.int32, (span, block), 0)
        query_pos = lax.broadcasted_iota(jnp.int32, (span, block), 1) + j * block
        attention = jnp.where(key_pos <= query_pos, jnp.exp(scores - stat), 0.0)
        grad_attention = nt_dot(v_ref[:span, :], g)
        grad_scores = (attention * (grad_attention - offset)).astype(jnp.bfloat16)
        dv_ref[:span, :] += jnp.dot(
            attention.astype(jnp.bfloat16), g, preferred_element_type=jnp.float32
        )
        dk_ref[:span, :] += jnp.dot(grad_scores, q, preferred_element_type=jnp.float32)
        dq_t = jnp.dot(kt_ref[:, :span], grad_scores, preferred_element_type=jnp.float32)
        dq_ref[rows, :] = (dq_t * scale).T.astype(dq_ref.dtype)

    @pl.when(head == pl.num_programs(0) - 1)
    def _():
        dkt_ref[...] = (dk_ref[...] * scale).T
        dvt_ref[...] = dv_ref[...].T


def attention_grads(query, key_one, value_one, attended, grad_att, stats):
    length, width = query.shape
    heads = width // HD
    per_head = pl.BlockSpec((length, HD), lambda h: (0, h))
    shared = pl.BlockSpec((length, HD), lambda h: (0, 0))
    flat = pl.BlockSpec((HD, length), lambda h: (0, 0))
    return pl.pallas_call(
        functools.partial(attention_kernel, 256),
        grid=(heads,),
        in_specs=[
            per_head,
            shared,
            flat,
            shared,
            per_head,
            per_head,
            pl.BlockSpec((heads, length), lambda h: (0, 0)),
        ],
        out_specs=[per_head, flat, flat],
        scratch_shapes=[pltpu.VMEM((length, HD), jnp.float32)] * 2,
        out_shape=[
            jax.ShapeDtypeStruct((length, width), jnp.bfloat16),
            jax.ShapeDtypeStruct((HD, length), jnp.float32),
            jax.ShapeDtypeStruct((HD, length), jnp.float32),
        ],
        compiler_params=pltpu.CompilerParams(
            dimension_semantics=("arbitrary",), vmem_limit_bytes=40 * 2**20
        ),
        cost_estimate=pl.CostEstimate(
            flops=10 * heads * length * length * HD,
            bytes_accessed=10 * length * width,
            transcendentals=heads * length * length,
        ),
        name="attention_grads",
    )(query, key_one, key_one.T, value_one, attended, grad_att, stats)


def projection_plain(grad_out, out_weight, attended):
    grad_rows = lax.all_gather(grad_out, "tensor", axis=0, tiled=True)
    grad_att = jnp.dot(
        grad_rows,
        lax.all_gather(out_weight, "dp", axis=0, tiled=True),
        preferred_element_type=jnp.float32,
    ).astype(jnp.bfloat16)
    weight_grad = lax.psum_scatter(
        lax.dot_general(
            grad_rows, attended, (((0,), (0,)), ((), ())), preferred_element_type=jnp.float32
        ).astype(jnp.bfloat16),
        "dp",
        scatter_dimension=0,
        tiled=True,
    )
    return grad_att, weight_grad


def tn_dot(a, b):
    return lax.dot_general(a, b, (((0,), (0,)), ((), ())), preferred_element_type=jnp.float32)


def fused_kernel(
    chips, g_hbm, w_hbm, q_hbm, k_hbm, v_hbm, a_hbm, s_hbm,
    dq_hbm, dk_out, dv_out, wg_hbm,
    big, att_all, w, q, k, v, kt, stats, own, part_out, part_in, ga, acc, wg,
    dq_acc, dq, dk, dv, kv_t, kv_out, kv_in, kv_done,
    load_sem, half_sem, g_sem, p_sem, a_sem, ga_sem, kv_sem,
    pair_send, right_send, left_send, first_send, a_send, ga_send, kv_send, dq_send, wg_send,
):
    dp = big.shape[1]
    unit, depth = big.shape[2], big.shape[3]
    local = unit // 2
    cols = w.shape[1]
    heads = cols // HD
    scale = HD ** (-0.5)
    last = 4 * chips
    me = lax.axis_index("dp")
    place = lax.axis_index("tensor")
    z, core = lax.div(place, 2), lax.rem(place, 2)
    mate = place + 1 - 2 * core
    my_y, my_x = lax.div(me, 2), lax.rem(me, 2)

    def other(j):
        return lax.rem(my_y + j // 2, 2) * 2 + lax.rem(my_x + j % 2, 2)

    def band(index, size):
        return pl.ds(pl.multiple_of(index * size, size), size)

    mine = pl.ds(pl.multiple_of(core * local, local), local)
    theirs = pl.ds(pl.multiple_of((1 - core) * local, local), local)

    def remote(source, target, send, recv, row, column):
        return pltpu.make_async_remote_copy(
            src_ref=source, dst_ref=target, send_sem=send, recv_sem=recv,
            device_id=(row, column), device_id_type=MESH,
        )

    key_head = lax.div(place * heads, GROUP)
    loads = [
        (g_hbm.at[:, band(me, depth)], big.at[z, me, mine, :], g_sem.at[z * dp + me]),
        (w_hbm, w, load_sem.at[0]),
        (a_hbm, att_all.at[me], load_sem.at[1]),
        (k_hbm.at[:, band(key_head, HD)], k, load_sem.at[2]),
        (v_hbm.at[:, band(key_head, HD)], v, load_sem.at[3]),
        (q_hbm, q, load_sem.at[4]),
        (s_hbm, stats, load_sem.at[5]),
    ]
    loads = [pltpu.make_async_copy(*each) for each in loads]
    for each in loads:
        each.start()

    barrier = pltpu.get_barrier_semaphore()

    def greet(row, column):
        pl.semaphore_signal(barrier, inc=1, device_id=(row, column), device_id_type=MESH)

    for j in range(1, dp):
        greet(other(j), place)
    greet(me, mate)
    greet(me, place + 2 - 4 * lax.rem(z, 2) + 1 - 2 * core)

    @pl.when(z > 0)
    def _():
        greet(me, place - 2)

    @pl.when(z < chips - 1)
    def _():
        greet(me, place + 2)

    acc[...] = jnp.zeros_like(acc)
    dk[...] = jnp.zeros_like(dk)
    dv[...] = jnp.zeros_like(dv)
    with jax.named_scope("loads"):
        for each in loads[1:]:
            each.wait()
    kt[...] = k[...].astype(jnp.float32).T.astype(jnp.bfloat16)

    edge = (z == 0).astype(jnp.int32) + (z == chips - 1).astype(jnp.int32)
    with jax.named_scope("barrier"):
        pl.semaphore_wait(barrier, dp + 3 - edge)

    def first_copy(j):
        return remote(
            g_hbm.at[:, band(other(j), depth)], big.at[z, me, mine, :],
            first_send, g_sem.at[z * dp + me], other(j), place,
        )

    def attended_copy(j, block):
        return remote(
            a_hbm.at[band(block, unit), :], att_all.at[me, band(block, unit), :],
            a_send, a_sem.at[me * chips + block], other(j), place,
        )

    def halves(part):
        return pl.ds(pl.multiple_of(core * local + part * (local // 2), local // 2), local // 2)

    def early_copy(part):
        return remote(
            g_hbm.at[pl.ds(part * (local // 2), local // 2), band(other(1), depth)],
            big.at[z, me, halves(part), :],
            first_send, half_sem if part else g_sem.at[z * dp + me],
            other(1), place,
        )

    early_copy(0).start()
    first_copy(2).start()
    early_copy(1).start()
    first_copy(3).start()
    for j in range(1, dp):
        attended_copy(j, z).start()

    def block_of(stage, side):
        block = z + (2 * side - 1) * stage
        inside = jnp.logical_and(block >= 0, block < chips)
        return block, jnp.logical_and(inside, jnp.logical_or(stage > 0, side == 0))

    def pair_copy(block, row):
        slot = block * dp + row
        chunk = big.at[block, row, mine, :]
        return remote(chunk, chunk, pair_send, p_sem.at[slot], me, mate)

    def right_copy(block, row):
        slot = block * dp + row
        chunk = big.at[block, row, mine, :]
        return remote(chunk, chunk, right_send.at[block], g_sem.at[slot], me, place + 2)

    def left_copy(block, row):
        slot = block * dp + row
        chunk = big.at[block, row, mine, :]
        return remote(chunk, chunk, left_send.at[block], g_sem.at[slot], me, place - 2)

    def part_copy(j, block, row):
        slot = (j - 1) * chips + block
        return remote(
            part_out.at[j - 1, band(block, unit), :], part_in.at[j - 1, band(block, unit), :],
            ga_send, ga_sem.at[slot], row, place,
        )

    def sides(stage, sub, body):
        def step(turn, carry):
            side = lax.select(jnp.logical_and(z == 1, stage > 0), 1 - turn, turn)
            block, valid = block_of(stage, side)

            @pl.when(valid)
            def _():
                swapped = jnp.logical_and(z == 0, stage > 1)
                place_of = (stage - 2) * dp + sub
                end = place_of == 2 * dp - 1
                early = jnp.logical_or(place_of < dp - 1, end)
                at = lax.select(swapped, lax.select(early, 2, 3), block)
                plain = lax.select(jnp.logical_or(at == 0, at == chips - 1), lax.rem(sub + 1, dp), sub)
                j = lax.select(
                    swapped,
                    lax.select(
                        end, 0,
                        lax.select(early, sub + 1, lax.rem(place_of - (dp - 1) + 1, dp)),
                    ),
                    plain,
                )
                row = lax.rem(my_y + lax.div(j, 2), 2) * 2 + lax.rem(my_x + lax.rem(j, 2), 2)
                body(side, at, j, row)

            return carry

        lax.fori_loop(0, 2, step, 0)

    def arrive(stage):
        def body(side, block, j, row):
            slot = block * dp + row
            held = jnp.logical_and(jnp.logical_and(z == 1, block == 2), j == 0)
            rightward = jnp.logical_and(side == 0, z < chips - 1)
            leftward = jnp.logical_and(jnp.logical_or(side == 1, stage == 0), z > 0)
            leftward = jnp.logical_and(leftward, jnp.logical_not(held))

            def pass_on(rows, sem):
                chunk = big.at[block, row, rows, :]
                with jax.named_scope("wait_chunk"):
                    remote(chunk, chunk, pair_send, sem, me, mate).wait_recv()

                @pl.when(rightward)
                def _():
                    remote(chunk, chunk, right_send.at[block], g_sem.at[slot], me, place + 2).start()

                @pl.when(leftward)
                def _():
                    remote(chunk, chunk, left_send.at[block], g_sem.at[slot], me, place - 2).start()

            early = jnp.logical_and(stage == 0, j == 1)

            @pl.when(early)
            def _():
                pass_on(halves(0), g_sem.at[slot])
                pass_on(halves(1), half_sem)

            @pl.when(jnp.logical_not(early))
            def _():
                pass_on(mine, g_sem.at[slot])

            pair_copy(block, row).start()

        return body

    def project(side, block, j, row):
        slot = block * dp + row
        chunk = big.at[block, row, theirs, :]
        with jax.named_scope("wait_mate"):
            remote(chunk, chunk, pair_send, p_sem.at[slot], me, mate).wait_recv()
        part = jnp.dot(big[block, row], w[...], preferred_element_type=jnp.float32)

        @pl.when(j == 0)
        def _():
            own[band(block, unit), :] = part

        @pl.when(j > 0)
        def _():
            part_out[j - 1, band(block, unit), :] = part.astype(jnp.bfloat16)

    def send_part(side, block, j, row):
        @pl.when(j > 0)
        def _():
            part_copy(j, block, row).start()

    def weight_term(side, block, j, row):
        @pl.when(j > 0)
        def _():
            rows = att_all.at[row, band(block, unit), :]
            slot = row * chips + block
            with jax.named_scope("wait_attended"):
                remote(rows, rows, a_send, a_sem.at[slot], me, mate).wait_recv()

        acc[...] += tn_dot(big[block, row], att_all[row, band(block, unit), :])

    ones = jnp.ones((8, HD), jnp.float32)

    width = HD // 4
    odd = lax.rem(z, 2)

    def strip(high, low_bit):
        return pl.ds(pl.multiple_of((high * 2 + low_bit) * width, width), width)

    beside = place + 2 - 4 * odd
    across = beside + 1 - 2 * core
    group = ((mate, odd, 1 - core), (beside, 1 - odd, core), (across, 1 - odd, 1 - core))

    def kv_store(tile):
        keys = band(tile, unit)
        kv_t[tile, 0] = (dk[keys, :] * scale).T
        kv_t[tile, 1] = dv[keys, :].T
        for number, (_, high, low_bit) in enumerate(group):
            for kind in range(2):
                kv_out[tile, number, kind] = kv_t[tile, kind, strip(high, low_bit), :].astype(jnp.bfloat16)

    def kv_copies(tile):
        return [
            remote(
                kv_out.at[tile, number], kv_in.at[tile, number],
                kv_send, kv_sem.at[tile * 3 + number], me, peer,
            )
            for number, (peer, _, _) in enumerate(group)
        ]

    def kv_start(tile):
        for each in kv_copies(tile):
            each.start()

    final_block = lax.select(z == 0, 2, lax.select(z == 1, chips - 1, 0))

    def attend(block):
        rows = band(block, unit)
        total = own[rows, :]
        for j in range(1, dp):
            with jax.named_scope("wait_part"):
                part_copy(j, block, me).wait_recv()
            total = total + part_in[j - 1, rows, :].astype(jnp.float32)
        ga[...] = total.astype(jnp.bfloat16)
        dq_acc[...] = jnp.zeros_like(dq_acc)
        offsets = []
        for h in range(heads):
            span = slice(h * HD, (h + 1) * HD)
            product = ga[:, span].astype(jnp.float32) * att_all[me, rows, span].astype(jnp.float32)
            offsets.append(
                lax.dot_general(
                    ones, product, (((1,), (1,)), ((), ())),
                    preferred_element_type=jnp.float32, precision=lax.Precision.HIGHEST,
                )[:1, :]
            )
        low = [stats[h : h + 1, rows] for h in range(heads)]

        def keys_tile(tile):
            keys = band(tile, unit)
            k_tile, v_tile, kt_tile = k[keys, :], v[keys, :], kt[:, keys]
            key_pos = lax.broadcasted_iota(jnp.int32, (unit, unit), 0) + tile * unit
            query_pos = lax.broadcasted_iota(jnp.int32, (unit, unit), 1) + block * unit
            allowed = key_pos <= query_pos
            dk_term, dv_term = dk[keys, :], dv[keys, :]
            for h in range(heads):
                span = slice(h * HD, (h + 1) * HD)
                q_tile, g_tile = q[rows, span], ga[:, span]
                scores = nt_dot(k_tile, q_tile) * scale
                attention = jnp.where(allowed, jnp.exp(scores - low[h]), 0.0)
                grad_attention = nt_dot(v_tile, g_tile)
                grad_scores = (attention * (grad_attention - offsets[h])).astype(jnp.bfloat16)
                dv_term += jnp.dot(
                    attention.astype(jnp.bfloat16), g_tile, preferred_element_type=jnp.float32
                )
                dk_term += jnp.dot(grad_scores, q_tile, preferred_element_type=jnp.float32)
                dq_acc[h] += jnp.dot(kt_tile, grad_scores, preferred_element_type=jnp.float32)
            dk[keys, :] = dk_term
            dv[keys, :] = dv_term

        final = block == final_block
        def keys_step(tile, carry):
            keys_tile(tile)

            @pl.when(final)
            def _():
                kv_store(tile)

                @pl.when(tile >= 1)
                def _():
                    kv_start(tile - 1)

            return carry

        lax.fori_loop(0, block + 1, keys_step, 0)
        for h in range(heads):
            dq[rows, h * HD : (h + 1) * HD] = (dq_acc[h] * scale).T.astype(dq.dtype)
        pltpu.make_async_copy(dq.at[rows, :], dq_hbm.at[rows, :], dq_send).start()

        @pl.when(final)
        def _():
            kv_start(block)

    def store_tile(tile, carry):
        kv_store(tile)
        return carry

    def start_tile(tile, carry):
        kv_start(tile)
        return carry

    def round_of(index, carry):
        @pl.when(index == last - 1)
        def _():
            lax.fori_loop(final_block + 1, chips, store_tile, 0)
            sides(chips - 1, dp - 2, weight_term)
            lax.fori_loop(final_block + 1, chips, start_tile, 0)

        stage, sub = lax.div(index, dp), lax.rem(index, dp)

        @pl.when(index < last)
        def _():
            sides(stage, sub, arrive(stage))

        @pl.when(jnp.logical_and(z == 1, index == 3 * dp - 1))
        def _():
            left_copy(2, me).start()

        @pl.when(jnp.logical_and(sub > 0, stage < chips - 1))
        def _():
            for side in range(2):
                block, valid = block_of(stage + 1, side)
                for j in range(1, dp):

                    @pl.when(jnp.logical_and(valid, sub == j))
                    def _(j=j, block=block):
                        attended_copy(j, block).start()

        @pl.when(index < last)
        def _():
            with jax.named_scope("project"):
                sides(stage, sub, project)

        @pl.when(jnp.logical_and(index > dp, index < last - 1))
        def _():
            with jax.named_scope("weight"):
                sides(lax.div(index - 1, dp), lax.rem(index - 1, dp), weight_term)

        @pl.when(jnp.logical_and(index >= dp, index < 2 * dp))
        def _():
            sides(0, sub, weight_term)

        @pl.when(index < last)
        def _():
            sides(stage, sub, send_part)

        attend_stage = (
            (index == 3 * dp).astype(jnp.int32)
            + 2 * (index == 3 * dp + 2).astype(jnp.int32)
            + 3 * (index == last).astype(jnp.int32)
        )

        @pl.when(jnp.logical_or(index == 2 * dp, attend_stage > 0))
        def _():
            with jax.named_scope("attend"):

                def step(side, carry):
                    block, valid = block_of(attend_stage, side)
                    swapped = lax.select(attend_stage == 2, 3, lax.select(attend_stage == 3, 2, attend_stage))

                    @pl.when(valid)
                    def _():
                        attend(lax.select(z == 0, swapped, block))

                    return carry

                lax.fori_loop(0, 2, step, 0)

        return carry

    lax.fori_loop(0, last + 1, round_of, 0)

    with jax.named_scope("weight_last"):
        sides(chips - 1, dp - 1, weight_term)
    pieces = 4
    piece = depth // pieces
    for index in range(pieces):
        rows = slice(index * piece, (index + 1) * piece)
        wg[rows, :] = acc[rows, :].astype(jnp.bfloat16)
        pltpu.make_async_copy(wg.at[rows, :], wg_hbm.at[rows, :], wg_send).start()

    def sent(ref, sem):
        remote(ref, ref, sem, kv_sem.at[0], me, mate).wait_send()

    with jax.named_scope("settle"):
        sent(big.at[:, :, mine, :], pair_send)
        for block in range(chips):

            @pl.when(jnp.logical_and(block <= z, z < chips - 1))
            def _(block=block):
                sent(big.at[block, :, mine, :], right_send.at[block])

            @pl.when(jnp.logical_and(block >= z, z > 0))
            def _(block=block):
                sent(big.at[block, :, mine, :], left_send.at[block])

        sent(big.at[0, pl.ds(0, dp - 1), mine, :], first_send)
        sent(att_all.at[pl.ds(0, dp - 1)], a_send)
        sent(part_out, ga_send)
        pltpu.make_async_copy(dq, dq_hbm, dq_send).wait()
        pltpu.make_async_copy(wg, wg_hbm, wg_send).wait()
    for tile in range(chips):
        for each in kv_copies(tile):
            with jax.named_scope("wait_kv"):
                each.wait_recv()
    with jax.named_scope("kv_sum"):
        for tile in range(chips):
            keys = slice(tile * unit, (tile + 1) * unit)
            for kind in range(2):
                total = kv_t[tile, kind, strip(odd, core), :]
                for number in range(3):
                    total = total + kv_in[tile, number, kind].astype(jnp.float32)
                kv_done[kind, :, keys] = total.astype(jnp.bfloat16)
    copies = [
        pltpu.make_async_copy(kv_done.at[kind], out, load_sem.at[kind])
        for kind, out in enumerate((dk_out, dv_out))
    ]
    for each in copies:
        each.start()
    sent(kv_out, kv_send)
    for each in copies:
        each.wait()


def finish_kernel(*refs):
    sources, targets, buffers, sems = refs[:4], refs[4:8], refs[8:12], refs[12:]
    pieces = ((3, 4), (0, 2), (1, 1), (2, 1))
    moves = []
    for index, count in pieces:
        size = sources[index].shape[0] // count
        for part in range(count):
            rows = pl.ds(part * size, size)
            slot = len(moves)
            moves.append(
                (
                    pltpu.make_async_copy(
                        sources[index].at[rows, :], buffers[index].at[rows, :], sems[0].at[slot]
                    ),
                    pltpu.make_async_copy(
                        buffers[index].at[rows, :], targets[index].at[rows, :], sems[1].at[slot]
                    ),
                )
            )
    for into, _ in moves:
        into.start()
    for into, out in moves:
        into.wait()
        out.start()
    for _, out in moves:
        out.wait()


def finish(*arrays):
    anywhere = pl.BlockSpec(memory_space=pl.ANY)
    shapes = [jax.ShapeDtypeStruct(each.shape, each.dtype) for each in arrays]
    return pl.pallas_call(
        finish_kernel,
        in_specs=[anywhere] * 4,
        out_specs=[anywhere] * 4,
        out_shape=shapes,
        scratch_shapes=[pltpu.VMEM(each.shape, each.dtype) for each in arrays]
        + [pltpu.SemaphoreType.DMA((8,)), pltpu.SemaphoreType.DMA((8,))],
        name="finish",
    )(*arrays)


def fused(grad_out, out_weight, query, keys, values, attended, stats):
    dp, tensor = lax.axis_size("dp"), lax.axis_size("tensor")
    chips = tensor // 2
    local = grad_out.shape[0]
    unit = 2 * local
    depth, cols = out_weight.shape
    length = query.shape[0]
    heads = cols // HD
    width = HD // 4
    low, wide = jnp.bfloat16, jnp.float32
    dma = pltpu.SemaphoreType.DMA
    anywhere = pl.BlockSpec(memory_space=pl.ANY)
    slots = chips * dp
    scratch = [
        pltpu.VMEM((chips, dp, unit, depth), low),
        pltpu.VMEM((dp, length, cols), low),
        pltpu.VMEM((depth, cols), low),
        pltpu.VMEM((length, cols), low),
        pltpu.VMEM((length, HD), low),
        pltpu.VMEM((length, HD), low),
        pltpu.VMEM((HD, length), low),
        pltpu.VMEM((heads, length), wide),
        pltpu.VMEM((length, cols), wide),
        pltpu.VMEM((dp - 1, length, cols), low),
        pltpu.VMEM((dp - 1, length, cols), low),
        pltpu.VMEM((unit, cols), low),
        pltpu.VMEM((depth, cols), wide),
        pltpu.VMEM((depth, cols), low),
        pltpu.VMEM((heads, HD, unit), wide),
        pltpu.VMEM((length, cols), low),
        pltpu.VMEM((length, HD), wide),
        pltpu.VMEM((length, HD), wide),
        pltpu.VMEM((chips, 2, HD, unit), wide),
        pltpu.VMEM((chips, 3, 2, width, unit), low),
        pltpu.VMEM((chips, 3, 2, width, unit), low),
        pltpu.VMEM((2, width, length), low),
        dma((6,)),
        dma,
        dma((slots,)),
        dma((slots,)),
        dma((slots,)),
        dma(((dp - 1) * chips,)),
        dma((3 * chips,)),
        dma,
        dma((chips,)),
        dma((chips,)),
        dma,
        dma,
        dma,
        dma,
        dma,
        dma,
    ]
    return pl.pallas_call(
        functools.partial(fused_kernel, chips),
        in_specs=[anywhere] * 7,
        out_specs=[anywhere] * 4,
        out_shape=[
            jax.ShapeDtypeStruct((length, cols), low),
            jax.ShapeDtypeStruct((width, length), low),
            jax.ShapeDtypeStruct((width, length), low),
            jax.ShapeDtypeStruct((depth, cols), low),
        ],
        scratch_shapes=scratch,
        compiler_params=pltpu.CompilerParams(
            collective_id=0, has_side_effects=True, vmem_limit_bytes=60 * 2**20
        ),
        cost_estimate=pl.CostEstimate(
            flops=4 * dp * length * depth * cols + 10 * length * length * cols,
            bytes_accessed=2 * slots * local * depth,
            transcendentals=heads * length * length,
        ),
        name="fused_grads",
    )(grad_out, out_weight, query, keys, values, attended, stats)


def per_device(grad_out, out_weight, query, keys, values, attended, stats):
    heads = query.shape[1] // HD
    if lax.axis_size("dp") == 4 and lax.axis_size("tensor") == 8 and heads * 4 == GROUP:
        query_grad, key_t, value_t, weight_grad = finish(
            *fused(grad_out, out_weight, query, keys, values, attended, stats)
        )
        return (query_grad, key_t.T, value_t.T, weight_grad)
    grad_att, weight_grad = projection_plain(grad_out, out_weight, attended)
    tensor_index = lax.axis_index("tensor")
    key_head = tensor_index * heads // GROUP
    key_one = lax.dynamic_slice_in_dim(keys, key_head * HD, HD, 1)
    value_one = lax.dynamic_slice_in_dim(values, key_head * HD, HD, 1)
    query_grad, key_part, value_part = attention_grads(
        query, key_one, value_one, attended, grad_att, stats
    )
    group_span = GROUP // heads
    group_place = tensor_index % group_span
    width, length = HD // group_span, query.shape[0]
    running_kv = jnp.stack([key_part, value_part]).reshape(2, group_span, width, length)
    for bit_number in range(group_span.bit_length() - 1):
        pairs = running_kv.reshape(2, -1, 2, width, length)
        odd = (group_place >> bit_number) % 2 == 1
        kept = jnp.where(odd, pairs[:, :, 1], pairs[:, :, 0])
        sent = jnp.where(odd, pairs[:, :, 0], pairs[:, :, 1])
        running_kv = kept + partner(
            sent.astype(jnp.bfloat16), "tensor", 1 << bit_number
        ).astype(sent.dtype)
    key_grad = running_kv[0, 0].T.astype(jnp.bfloat16)
    value_grad = running_kv[1, 0].T.astype(jnp.bfloat16)
    return (query_grad, key_grad, value_grad, weight_grad)


def solution(mesh):
    placed = (
        P(("dp", "tensor"), None),
        P("dp", "tensor"),
        P("dp", "tensor"),
        P("dp", None),
        P("dp", None),
        P("dp", "tensor"),
        P("tensor", "dp"),
    )
    return jax.shard_map(
        per_device,
        mesh=mesh,
        in_specs=placed,
        out_specs=(P("dp", "tensor"), P("dp", "tensor"), P("dp", "tensor"), P("dp", "tensor")),
        check_vma=False,
    )
```
